256 devices in a mesh: band: 16 (over y_hi, z), grid: 16 (over y_lo, x, core).
Axes of the slice: x: 4, y: 4 (y_hi: 2, y_lo: 2; y = y_hi * 2 + y_lo), z: 8, core: 2. Of those that a mesh axis runs over, the one named last changes fastest.
Arguments:
- own_bands: float32 [64, 128, 128, 128], P('band', 'grid'), may hold values from -1.5 to 1.5
- travel_bands: float32 [64, 128, 128, 128], P('band', 'grid'), may hold values from -1.5 to 1.5
Outputs:
- own_terms: float32 [64, 128, 128, 128], P('band', 'grid')
- partner_terms: float32 [64, 128, 128, 128], P('band', 'grid')
The draws below stay inside these ranges and needn't reach their ends.
All inputs are finite; a program needn't handle non-finite values.
Results may differ from the reference program's by a relative error of at most 0.00011.
Values sent between devices are 32-bit elements; how exact they have to be, the bound alone decides.
A program may use at most 64 MiB of HBM per device.

```python
import math
import jax
import jax.numpy as jnp
from jax import lax

NX = 128
NY = 128
NZ = 128
OWN = 4
VIS = 4
BANDS = 64
TRAVEL = 64
N_BAND = 16


def band_field(base_key, band_count):
    return 0.5 * jax.random.truncated_normal(jax.random.fold_in(base_key, 4), -3.0, 3.0, (band_count, NZ, NY, NX), jnp.float32)


def draw_own_bands(key, part):
    return band_field(jax.random.fold_in(key, 11), BANDS)


def draw_travel_bands(key, part):
    return band_field(jax.random.fold_in(key, 23), TRAVEL)


def setup_inputs(seed: int = 0) -> dict:
    streams_of = jax.random.split(jax.random.key(seed), 3)
    return {
        "own_bands": draw_own_bands(jax.random.fold_in(streams_of[2], 71), 0),
        "travel_bands": draw_travel_bands(jax.random.fold_in(streams_of[2], 71), 0),
    }


FRACTION = 0.25


def wave_square(points, first_row, length):
    position = first_row + jnp.arange(points, dtype=jnp.int32)
    position = (position + length // 2) % length - length // 2
    wavenumber = (2.0 * math.pi / length) * position.astype(jnp.float32)
    return wavenumber * wavenumber


def coulomb(first_row, row_count):
    squared = wave_square(NZ, 0, NZ)[:, None, None] + wave_square(row_count, first_row, NY)[None, :, None] + wave_square(NX, 0, NX)[None, None, :]
    safe_square = jnp.where(squared > 0.0, squared, 1.0)
    return jnp.where(squared > 0.0, 4.0 * math.pi / safe_square, 0.0)


def reference(own_bands, travel_bands):
    kernel = coulomb(0, NY)[:, :, : NX // 2 + 1]
    owned_groups = own_bands.reshape(N_BAND, OWN, NZ, NY, NX)
    arrived = jnp.roll(travel_bands.reshape(N_BAND, VIS, NZ, NY, NX), 1, axis=0)

    def group_terms(blocks):
        owned, visitors = blocks

        def visit_band(accumulated, visitor):
            density = owned * visitor
            potential = jnp.fft.irfftn(kernel * jnp.fft.rfftn(density, axes=(1, 2, 3)), s=(NZ, NY, NX), axes=(1, 2, 3))
            return accumulated + potential * visitor, jnp.sum(potential * owned, axis=0)

        accumulated, partner = lax.scan(visit_band, jnp.zeros_like(owned), visitors)
        return -FRACTION * accumulated, -FRACTION * partner

    own_terms, held = lax.map(group_terms, (owned_groups, arrived))
    held = jnp.roll(held, -1, axis=0)
    return own_terms.reshape(BANDS, NZ, NY, NX), held.reshape(TRAVEL, NZ, NY, NX)
```

```python
import functools
import math

import jax
import jax.numpy as jnp
import ml_dtypes
import numpy as np
from jax import lax
from jax.experimental import pallas as pl
from jax.experimental.pallas import tpu as pltpu
from jax.sharding import PartitionSpec as P

N = 128
FRACTION = 0.25
ROW = 8
KYS = N // ROW
LOCAL = 8
VIS = 4
PAIRED = 2
BLOCK = LOCAL * KYS
PAIR_ROWS = 2 * ROW * BLOCK
STEPS = ((2, 0), (2, 1), (1, 0), (3, 0), (1, 1), (3, 1), (0, 1))
F32 = jnp.float32
BF16 = jnp.bfloat16
MESH = pl.DeviceIdType.MESH


def real_basis():
    n = np.arange(N)
    rows = []
    for m in range(N):
        if m <= N // 2:
            row = np.cos(2.0 * np.pi * ((m * n) % N) / N)
        else:
            row = np.sin(2.0 * np.pi * (((N - m) * n) % N) / N)
        scale = 1.0 / N if m in (0, N // 2) else 2.0 / N
        rows.append(np.sqrt(scale) * row)
    return np.stack(rows)


def high_low(table):
    high = table.astype(np.float32).astype(ml_dtypes.bfloat16)
    low = (table - high.astype(np.float64)).astype(np.float32).astype(ml_dtypes.bfloat16)
    return high, low


def tables():
    basis = real_basis()
    high, low = high_low(basis)
    high_t, low_t = high.T, low.T
    from_left = np.block([[high, high], [low, low]])
    from_left_inverse = np.block([[high_t, high_t], [low_t, low_t]])
    from_right = np.block([[high_t, low_t], [high_t, low_t]])
    from_right_inverse = np.block([[high, low], [high, low]])
    return [from_left, from_left_inverse, from_right, from_right_inverse]


def halves(value, axis):
    high = value.astype(BF16)
    low = (value - high.astype(F32)).astype(BF16)
    return jnp.concatenate([high, low], axis=axis)


def along_rows(table, value):
    both = jnp.dot(table, halves(value, 0), preferred_element_type=F32)
    return both[:N] + both[N:]


def along_lanes(value, table):
    both = jnp.dot(halves(value, 1), table, preferred_element_type=F32)
    return both[:, :N] + both[:, N:]


def wave_square(position):
    position = lax.rem(position + N // 2, N) - N // 2
    number = 2.0 * math.pi / N * position.astype(F32)
    return number * number


def kernel(
    own, travel, lt_ref, lti_ref, wx_ref, wxi_ref, own_out, held_out,
    ownb, visb, send, recv, back, own_sum, held, held_part, coulomb,
    load_sem, exch_send, exch_recv, vis_send, vis_recv, relay_send, relay_recv,
    fwd_send, fwd_recv, bwd_send, bwd_recv,
    part_send, part_recv, out_send, out_recv, ret_send, ret_recv, store_sem,
):
    band = lax.axis_index("band")
    groups = lax.axis_size("band")
    grid = lax.axis_index("grid")
    mine = grid // ROW
    other = 1 - mine
    place = grid % ROW
    x, core = place // 2, place % 2
    partner = {"grid": other * ROW + place}
    ahead = {"band": (band + 1) % groups}
    behind = {"band": (band + groups - 1) % groups}
    places = [((x + dx) % 4) * 2 + (core + dc) % 2 for dx, dc in STEPS]
    peers = [{"grid": mine * ROW + p} for p in places]

    def remote(src, dst, send_sem, recv_sem, device):
        return pltpu.make_async_remote_copy(
            src_ref=src, dst_ref=dst, send_sem=send_sem, recv_sem=recv_sem,
            device_id=device, device_id_type=MESH,
        )

    for i in range(PAIRED):
        pltpu.make_async_copy(own.at[2 * mine + i], ownb.at[i, mine], load_sem.at[i]).start()

    barrier = pltpu.get_barrier_semaphore()
    for device in [ahead, behind, partner] + peers:
        pl.semaphore_signal(barrier, inc=1, device_id=device, device_id_type=MESH)
    pl.semaphore_wait(barrier, 3 + len(peers))

    def visitor(j, q):
        return remote(
            travel.at[j, pl.ds(2 * q, 2)], visb.at[j, mine, pl.ds(2 * q, 2)],
            vis_send.at[j, q], vis_recv.at[j, q], ahead,
        )

    def relay(j, q, half):
        return remote(
            visb.at[j, half, pl.ds(2 * q, 2)], visb.at[j, half, pl.ds(2 * q, 2)],
            relay_send.at[j, q], relay_recv.at[j, q], partner,
        )

    def exchange(i, half, index):
        return remote(own.at[index], ownb.at[i, half], exch_send.at[i], exch_recv.at[i], partner)

    for j in range(VIS):
        for q in range(4):
            visitor(j, q).start()
        if j == 0:
            for i in range(PAIRED):
                exchange(i, mine, 2 * other + i).start()

    kz = lax.broadcasted_iota(jnp.int32, (N, 2 * N), 0)
    lane = lax.broadcasted_iota(jnp.int32, (N, 2 * N), 1)
    kx_square = wave_square(lax.rem(lane, N))
    kz_square = wave_square(kz)

    def fill(kp, carry):
        ky = place * KYS + 2 * kp + lane // N
        squared = kz_square + wave_square(ky) + kx_square
        safe = jnp.where(squared > 0.0, squared, 1.0)
        value = jnp.where(squared > 0.0, 4.0 * math.pi / safe, 0.0)
        coulomb[kp] = -FRACTION * value
        return carry

    lax.fori_loop(0, KYS // 2, fill, 0)

    def base(j, i, half, p):
        return ((j * PAIRED + i) * 2 + half) * ROW * BLOCK + p * BLOCK

    def rows(ref, start, count):
        return ref.at[pl.ds(pl.multiple_of(start, KYS), count)]

    def forward(j, half, own_half):
        def piece(q, carry):
            if own_half:
                visitor(j, q).wait_recv()
                relay(j, q, mine).start()
            else:
                relay(j, q, other).wait_recv()
            planes = pl.ds(2 * q, 2)
            vis = visb[j, half, planes].reshape(2 * N, N)
            for i in range(PAIRED):
                density = ownb[i, half, planes].reshape(2 * N, N) * vis
                wave = along_lanes(density, wx_ref[...])
                wave = jnp.concatenate([wave[:N], wave[N:]], axis=1)
                wave = along_rows(lt_ref[...], wave)
                for p in range(ROW):
                    for z in range(2):
                        start = base(j, i, half, p) + (2 * q + z) * KYS
                        send[pl.ds(pl.multiple_of(start, KYS), KYS), :] = wave[
                            p * KYS : (p + 1) * KYS, z * N : (z + 1) * N
                        ]
                start = pl.multiple_of(base(j, i, half, place) + 2 * q * KYS, KYS)
                recv[pl.ds(start, 2 * KYS), :] = send[pl.ds(start, 2 * KYS), :]
            for i in range(PAIRED):
                for p, peer in zip(places, peers):
                    remote(
                        rows(send, base(j, i, half, p) + 2 * q * KYS, 2 * KYS),
                        rows(recv, base(j, i, half, place) + 2 * q * KYS, 2 * KYS),
                        fwd_send, fwd_recv.at[j, half], peer,
                    ).start()
            return carry

        lax.fori_loop(0, 4, piece, 0)

    def screen(j):
        for half in (mine, other):
            whole = rows(recv, 0, (ROW - 1) * PAIRED * BLOCK)
            remote(whole, whole, fwd_send, fwd_recv.at[j, half], partner).wait_recv()

        def columns(step, carry):
            i, kp = step // (KYS // 2), step % (KYS // 2)
            start = (j * PAIRED + i) * PAIR_ROWS + 2 * kp
            first = pl.ds(start, N, stride=KYS)
            second = pl.ds(start + 1, N, stride=KYS)
            wave = jnp.concatenate([recv[first, :], recv[second, :]], axis=1)
            wave = along_rows(lt_ref[...], wave) * coulomb[kp]
            wave = along_rows(lti_ref[...], wave)
            recv[first, :] = wave[:, :N]
            recv[second, :] = wave[:, N:]
            return carry

        lax.fori_loop(0, PAIRED * KYS // 2, columns, 0)
        for i in range(PAIRED):
            for half in range(2):
                start = pl.multiple_of(base(j, i, half, place), KYS)
                back[pl.ds(start, BLOCK), :] = recv[pl.ds(start, BLOCK), :]
        for half in (other, mine):
            for zq in range(2):
                for i in range(PAIRED):
                    for p, peer in zip(places, peers):
                        remote(
                            rows(recv, base(j, i, half, p) + zq * (BLOCK // 2), BLOCK // 2),
                            rows(back, base(j, i, half, place) + zq * (BLOCK // 2), BLOCK // 2),
                            bwd_send, bwd_recv.at[j, half, zq], peer,
                        ).start()

    def inverse(j, half, zq):
        whole = rows(back, 0, (ROW - 1) * PAIRED * (BLOCK // 2))
        remote(whole, whole, bwd_send, bwd_recv.at[j, half, zq], partner).wait_recv()

        def planes_of(step, carry):
            zp, i = step // PAIRED, step % PAIRED
            z = 4 * zq + 2 * zp
            sides = []
            for k in range(2):
                parts = []
                for p in range(ROW):
                    start = base(j, i, half, p) + (z + k) * KYS
                    parts.append(back[pl.ds(pl.multiple_of(start, KYS), KYS), :])
                sides.append(jnp.concatenate(parts, axis=0))
            wave = along_rows(lti_ref[...], jnp.concatenate(sides, axis=1))
            wave = jnp.concatenate([wave[:, :N], wave[:, N:]], axis=0)
            potential = along_lanes(wave, wxi_ref[...]).reshape(2, N, N)
            planes = pl.ds(z, 2)
            own_part = potential * visb[j, half, planes]
            if j > 0:
                own_part = own_part + own_sum[i, half, planes]
            own_sum[i, half, planes] = own_part
            held_term = potential * ownb[i, half, planes]

            @pl.when(i == 0)
            def _():
                held[j, half, planes] = held_term

            @pl.when(i > 0)
            def _():
                held[j, half, planes] = held[j, half, planes] + held_term

            return carry

        lax.fori_loop(0, 2 * PAIRED, planes_of, 0)

    def partial(j, zq):
        planes = pl.ds(4 * zq, 4)
        return remote(
            held.at[j, other, planes], held_part.at[j, planes],
            part_send.at[j, zq], part_recv.at[j, zq], partner,
        )

    def outgoing(j, zq):
        planes = pl.ds(4 * zq, 4)
        return remote(
            held.at[j, mine, planes], held_out.at[j, planes],
            out_send.at[j, zq], out_recv.at[j, zq], behind,
        )

    def returned(i, zq):
        planes = pl.ds(4 * zq, 4)
        return remote(
            own_sum.at[i, other, planes], own_out.at[2 * mine + i, planes],
            ret_send.at[i, zq], ret_recv.at[i, zq], partner,
        )

    def stored(i, zq):
        planes = pl.ds(4 * zq, 4)
        return pltpu.make_async_copy(
            own_sum.at[i, mine, planes], own_out.at[2 * mine + i, planes], store_sem.at[i, zq]
        )

    def back_part(j):
        for zq in range(2):
            inverse(j, other, zq)
            partial(j, zq).start()
            if j == VIS - 1:
                for i in range(PAIRED):
                    returned(i, zq).start()
        for zq in range(2):
            inverse(j, mine, zq)
            if j == VIS - 1:
                for i in range(PAIRED):
                    stored(i, zq).start()
                settle(j, zq)

    def settle(j, zq):
        partial(j, zq).wait_recv()
        planes = pl.ds(4 * zq, 4)
        held[j, mine, planes] = held[j, mine, planes] + held_part[j, planes]
        outgoing(j, zq).start()

    def settle_all(j):
        for zq in range(2):
            settle(j, zq)

    for i in range(PAIRED):
        pltpu.make_async_copy(own.at[2 * mine + i], ownb.at[i, mine], load_sem.at[i]).wait()
    forward(0, mine, True)
    forward(1, mine, True)
    forward(2, mine, True)
    for i in range(PAIRED):
        exchange(i, other, 2 * mine + i).wait_recv()
    forward(0, other, False)
    forward(3, mine, True)
    screen(0)
    forward(1, other, False)
    forward(2, other, False)
    screen(1)
    back_part(0)
    forward(3, other, False)
    screen(2)
    settle_all(0)
    back_part(1)
    screen(3)
    settle_all(1)
    back_part(2)
    settle_all(2)
    back_part(3)

    for j in range(VIS):
        for q in range(4):
            visitor(j, q).wait_send()
            relay(j, q, mine).wait_send()
    for i in range(PAIRED):
        exchange(i, mine, 2 * other + i).wait_send()
    sent = rows(send, 0, (ROW - 1) * PAIRED * 2 * VIS * BLOCK)
    remote(sent, sent, fwd_send, fwd_recv.at[0, 0], partner).wait_send()
    remote(sent, sent, bwd_send, fwd_recv.at[0, 0], partner).wait_send()
    for zq in range(2):
        for j in range(VIS):
            partial(j, zq).wait_send()
            outgoing(j, zq).wait()
        for i in range(PAIRED):
            returned(i, zq).wait()
            stored(i, zq).wait()


def body(own_bands, travel_bands):
    table_list = [jnp.asarray(t) for t in tables()]
    whole = 4 * PAIR_ROWS * PAIRED
    dma = pltpu.SemaphoreType.DMA
    any_space = pl.BlockSpec(memory_space=pl.ANY)
    vmem = pl.BlockSpec(memory_space=pltpu.VMEM)
    return pl.pallas_call(
        kernel,
        out_shape=[
            jax.ShapeDtypeStruct(own_bands.shape, F32),
            jax.ShapeDtypeStruct(travel_bands.shape, F32),
        ],
        in_specs=[any_space, any_space] + [vmem] * 4,
        out_specs=[any_space, any_space],
        scratch_shapes=[
            pltpu.VMEM((PAIRED, 2, LOCAL, N, N), F32),
            pltpu.VMEM((VIS, 2, LOCAL, N, N), F32),
            pltpu.VMEM((whole, N), F32),
            pltpu.VMEM((whole, N), F32),
            pltpu.VMEM((whole, N), F32),
            pltpu.VMEM((PAIRED, 2, LOCAL, N, N), F32),
            pltpu.VMEM((VIS, 2, LOCAL, N, N), F32),
            pltpu.VMEM((VIS, LOCAL, N, N), F32),
            pltpu.VMEM((KYS // 2, N, 2 * N), F32),
            dma((PAIRED,)),
            dma((PAIRED,)),
            dma((PAIRED,)),
            dma((VIS, 4)),
            dma((VIS, 4)),
            dma((VIS, 4)),
            dma((VIS, 4)),
            dma,
            dma((VIS, 2)),
            dma,
            dma((VIS, 2, 2)),
            dma((VIS, 2)),
            dma((VIS, 2)),
            dma((VIS, 2)),
            dma((VIS, 2)),
            dma((PAIRED, 2)),
            dma((PAIRED, 2)),
            dma((PAIRED, 2)),
        ],
        compiler_params=pltpu.CompilerParams(
            collective_id=0, has_side_effects=True, vmem_limit_bytes=60 * 2**20
        ),
        name="exchange_terms",
    )(own_bands, travel_bands, *table_list)


def solution(mesh):
    in_specs = (P("band", "grid", None, None), P("band", "grid", None, None))
    out_specs = (P("band", "grid", None, None), P("band", "grid", None, None))
    return jax.shard_map(body, mesh=mesh, in_specs=in_specs, out_specs=out_specs, check_vma=False)
```

```python
import functools
import math

import jax
import jax.numpy as jnp
import ml_dtypes
import numpy as np
from jax import lax
from jax.experimental import pallas as pl
from jax.experimental.pallas import tpu as pltpu
from jax.sharding import PartitionSpec as P

N = 128
FRACTION = 0.25
ROW = 8
KYS = N // ROW
LOCAL = 8
COLUMN = 8
AHEAD = 1
VIS = 4
PAIRED = 2
BLOCK = LOCAL * KYS
PAIR_ROWS = 2 * ROW * BLOCK
STEPS = ((2, 0), (2, 1), (1, 0), (3, 0), (1, 1), (3, 1), (0, 1))
F32 = jnp.float32
BF16 = jnp.bfloat16
MESH = pl.DeviceIdType.MESH


def real_basis():
    n = np.arange(N)
    rows = []
    for m in range(N):
        if m <= N // 2:
            row = np.cos(2.0 * np.pi * ((m * n) % N) / N)
        else:
            row = np.sin(2.0 * np.pi * (((N - m) * n) % N) / N)
        scale = 1.0 / N if m in (0, N // 2) else 2.0 / N
        rows.append(np.sqrt(scale) * row)
    return np.stack(rows)


def high_low(table):
    high = table.astype(np.float32).astype(ml_dtypes.bfloat16)
    low = (table - high.astype(np.float64)).astype(np.float32).astype(ml_dtypes.bfloat16)
    return high, low


def tables():
    basis = real_basis()
    high, low = high_low(basis)
    high_t, low_t = high.T, low.T
    from_left = np.block([[high, high], [low, low]])
    from_left_inverse = np.block([[high_t, high_t], [low_t, low_t]])
    from_right = np.block([[high_t, low_t], [high_t, low_t]])
    from_right_inverse = np.block([[high, low], [high, low]])
    return [from_left, from_left_inverse, from_right, from_right_inverse]


def halves(value, axis):
    high = value.astype(BF16)
    low = (value - high.astype(F32)).astype(BF16)
    return jnp.concatenate([high, low], axis=axis)


def along_rows(table, value):
    both = jnp.dot(table, halves(value, 0), preferred_element_type=F32)
    return both[:N] + both[N:]


def along_lanes(value, table):
    both = jnp.dot(halves(value, 1), table, preferred_element_type=F32)
    return both[:, :N] + both[:, N:]


def wave_square(position):
    position = lax.rem(position + N // 2, N) - N // 2
    number = 2.0 * math.pi / N * position.astype(F32)
    return number * number


def kernel(
    own, travel, lt_ref, lti_ref, wx_ref, wxi_ref, own_out, held_out,
    ownb, visb, send, recv, back, own_sum, held, held_part, coulomb,
    load_sem, exch_send, exch_recv, vis_send, vis_recv, relay_send, relay_recv,
    fwd_send, fwd_recv, bwd_send, bwd_recv,
    part_send, part_recv, out_send, out_recv, ret_send, ret_recv, store_sem,
):
    band = lax.axis_index("band")
    groups = lax.axis_size("band")
    grid = lax.axis_index("grid")
    mine = grid // ROW
    other = 1 - mine
    place = grid % ROW
    x, core = place // 2, place % 2
    partner = {"grid": other * ROW + place}
    ahead_band = (band + 1) % groups
    turn = (COLUMN - band % COLUMN) // COLUMN
    ahead_turn = (COLUMN - ahead_band % COLUMN) // COLUMN
    direct = (mine + turn) % 2
    passed = 1 - direct
    ahead = {"band": ahead_band, "grid": (mine + ahead_turn) % 2 * ROW + place}
    behind = {"band": (band + groups - 1) % groups, "grid": direct * ROW + place}
    places = [((x + dx) % 4) * 2 + (core + dc) % 2 for dx, dc in STEPS]
    peers = [{"grid": mine * ROW + p} for p in places]

    def remote(src, dst, send_sem, recv_sem, device):
        return pltpu.make_async_remote_copy(
            src_ref=src, dst_ref=dst, send_sem=send_sem, recv_sem=recv_sem,
            device_id=device, device_id_type=MESH,
        )

    for i in range(PAIRED):
        pltpu.make_async_copy(own.at[2 * mine + i], ownb.at[i, mine], load_sem.at[i]).start()

    barrier = pltpu.get_barrier_semaphore()
    for device in [ahead, behind, partner] + peers:
        pl.semaphore_signal(barrier, inc=1, device_id=device, device_id_type=MESH)
    pl.semaphore_wait(barrier, 3 + len(peers))

    def visitor(j, q):
        return remote(
            travel.at[j, pl.ds(2 * q, 2)], visb.at[j, mine, pl.ds(2 * q, 2)],
            vis_send, vis_recv.at[j, q], ahead,
        )

    def relay(j, q, half):
        return remote(
            visb.at[j, half, pl.ds(2 * q, 2)], visb.at[j, half, pl.ds(2 * q, 2)],
            relay_send, relay_recv.at[j, q], partner,
        )

    def exchange(i, q, half, index):
        return remote(
            own.at[index, pl.ds(2 * q, 2)], ownb.at[i, half, pl.ds(2 * q, 2)],
            exch_send, exch_recv.at[i, q], partner,
        )

    def hand_over(i):
        for q in range(4):
            exchange(i, q, mine, 2 * other + i).start()

    for j in range(VIS):
        for q in range(4):
            visitor(j, q).start()

    @pl.when(turn == 0)
    def _():
        hand_over(0)

    kz = lax.broadcasted_iota(jnp.int32, (N, 2 * N), 0)
    lane = lax.broadcasted_iota(jnp.int32, (N, 2 * N), 1)
    kx_square = wave_square(lax.rem(lane, N))
    kz_square = wave_square(kz)

    def fill(kp, carry):
        ky = place * KYS + 2 * kp + lane // N
        squared = kz_square + wave_square(ky) + kx_square
        safe = jnp.where(squared > 0.0, squared, 1.0)
        value = jnp.where(squared > 0.0, 4.0 * math.pi / safe, 0.0)
        coulomb[kp] = -FRACTION * value
        return carry

    lax.fori_loop(0, KYS // 2, fill, 0)

    def base(j, i, half, p):
        return ((j * PAIRED + i) * 2 + half) * ROW * BLOCK + p * BLOCK

    def rows(ref, start, count):
        return ref.at[pl.ds(pl.multiple_of(start, KYS), count)]

    def pass_on(index):
        j, q = index // 4, index % 4
        visitor(j, q).wait_recv()
        relay(j, q, direct).start()

    def transform(j, i, half, q):
        planes = pl.ds(2 * q, 2)
        density = (ownb[i, half, planes] * visb[j, half, planes]).reshape(2 * N, N)
        wave = along_lanes(density, wx_ref[...])
        wave = jnp.concatenate([wave[:N], wave[N:]], axis=1)
        wave = along_rows(lt_ref[...], wave)
        for p in range(ROW):
            for z in range(2):
                start = base(j, i, half, p) + (2 * q + z) * KYS
                send[pl.ds(pl.multiple_of(start, KYS), KYS), :] = wave[
                    p * KYS : (p + 1) * KYS, z * N : (z + 1) * N
                ]
        start = pl.multiple_of(base(j, i, half, place) + 2 * q * KYS, KYS)
        recv[pl.ds(start, 2 * KYS), :] = send[pl.ds(start, 2 * KYS), :]
        for p, peer in zip(places, peers):
            remote(
                rows(send, base(j, i, half, p) + 2 * q * KYS, 2 * KYS),
                rows(recv, base(j, i, half, place) + 2 * q * KYS, 2 * KYS),
                fwd_send, fwd_recv.at[j, half], peer,
            ).start()

    def forward_mine(first, last):
        def piece(step, carry):
            j, q = step // 4, step % 4
            index = step + AHEAD * turn

            @pl.when(index < 4 * VIS)
            def _():
                pass_on(index)

            @pl.when(turn == 1)
            def _():
                relay(j, q, passed).wait_recv()

            for i in range(PAIRED):
                transform(j, i, mine, q)
            return carry

        lax.fori_loop(4 * first, 4 * last, piece, 0)

    def forward_other(visitors, fresh):
        def piece(step, carry):
            i, q = step // 4, step % 4
            if fresh:
                exchange(i, q, other, 2 * mine + i).wait_recv()

            @pl.when((turn == 0) & (i == 0))
            def _():
                for j in visitors:
                    relay(j, q, passed).wait_recv()

            for j in visitors:
                transform(j, i, other, q)
            return carry

        lax.fori_loop(0, 4 * PAIRED, piece, 0)

    def screen(j):
        for half in (mine, other):
            whole = rows(recv, 0, (ROW - 1) * PAIRED * BLOCK)
            remote(whole, whole, fwd_send, fwd_recv.at[j, half], partner).wait_recv()

        def columns(step, carry):
            i, kp = step // (KYS // 2), step % (KYS // 2)
            start = (j * PAIRED + i) * PAIR_ROWS + 2 * kp
            first = pl.ds(start, N, stride=KYS)
            second = pl.ds(start + 1, N, stride=KYS)
            wave = jnp.concatenate([recv[first, :], recv[second, :]], axis=1)
            wave = along_rows(lt_ref[...], wave) * coulomb[kp]
            wave = along_rows(lti_ref[...], wave)
            recv[first, :] = wave[:, :N]
            recv[second, :] = wave[:, N:]
            return carry

        lax.fori_loop(0, PAIRED * KYS // 2, columns, 0)
        for i in range(PAIRED):
            for half in range(2):
                start = pl.multiple_of(base(j, i, half, place), KYS)
                back[pl.ds(start, BLOCK), :] = recv[pl.ds(start, BLOCK), :]

    def give_back(visitors, half):
        def piece(q, carry):
            for j in visitors:
                for i in range(PAIRED):
                    for p, peer in zip(places, peers):
                        remote(
                            rows(recv, base(j, i, half, p) + 2 * q * KYS, 2 * KYS),
                            rows(back, base(j, i, half, place) + 2 * q * KYS, 2 * KYS),
                            bwd_send, bwd_recv.at[j, half, q], peer,
                        ).start()
            return carry

        lax.fori_loop(0, 4, piece, 0)

    def inverse(j, half, q):
        whole = rows(back, 0, (ROW - 1) * PAIRED * 2 * KYS)
        remote(whole, whole, bwd_send, bwd_recv.at[j, half, q], partner).wait_recv()
        planes = pl.ds(2 * q, 2)
        held_term = None
        for i in range(PAIRED):
            sides = []
            for k in range(2):
                parts = []
                for p in range(ROW):
                    start = base(j, i, half, p) + (2 * q + k) * KYS
                    parts.append(back[pl.ds(pl.multiple_of(start, KYS), KYS), :])
                sides.append(jnp.concatenate(parts, axis=0))
            wave = along_rows(lti_ref[...], jnp.concatenate(sides, axis=1))
            wave = jnp.concatenate([wave[:, :N], wave[:, N:]], axis=0)
            potential = along_lanes(wave, wxi_ref[...]).reshape(2, N, N)
            own_part = potential * visb[j, half, planes]
            if j > 0:
                own_part = own_part + own_sum[i, half, planes]
            own_sum[i, half, planes] = own_part
            term = potential * ownb[i, half, planes]
            held_term = term if held_term is None else held_term + term
        held[j, half, planes] = held_term

    def partial(j, q):
        planes = pl.ds(2 * q, 2)
        return remote(
            held.at[j, passed, planes], held_part.at[j, planes],
            part_send, part_recv.at[j, q], partner,
        )

    def outgoing(j, q):
        planes = pl.ds(2 * q, 2)
        return remote(
            held.at[j, direct, planes], held_out.at[j, planes],
            out_send, out_recv, behind,
        )

    def returned(i, q):
        planes = pl.ds(2 * q, 2)
        return remote(
            own_sum.at[i, other, planes], own_out.at[2 * mine + i, planes],
            ret_send, ret_recv, partner,
        )

    def stored(i, q):
        planes = pl.ds(2 * q, 2)
        return pltpu.make_async_copy(
            own_sum.at[i, mine, planes], own_out.at[2 * mine + i, planes], store_sem.at[i, q]
        )

    def settle(j, q):
        partial(j, q).wait_recv()
        planes = pl.ds(2 * q, 2)
        held[j, direct, planes] = held[j, direct, planes] + held_part[j, planes]
        outgoing(j, q).start()

    def back_other(visitors):
        def piece(q, carry):
            for j in visitors:
                inverse(j, other, q)

                @pl.when(turn == 0)
                def _():
                    partial(j, q).start()

            if VIS - 1 in visitors:
                for i in range(PAIRED):
                    returned(i, q).start()
            return carry

        lax.fori_loop(0, 4, piece, 0)

    def back_mine(j):
        def piece(q, carry):
            inverse(j, mine, q)
            if j == VIS - 1:
                for i in range(PAIRED):
                    stored(i, q).start()

            @pl.when(turn == 0)
            def _():
                settle(j, q)

            @pl.when(turn == 1)
            def _():
                partial(j, q).start()
                index = 4 * j + q - 1

                @pl.when(index >= 0)
                def _():
                    settle(index // 4, index % 4)

            return carry

        lax.fori_loop(0, 4, piece, 0)

    @pl.when(turn == 1)
    def _():
        lax.fori_loop(0, AHEAD, lambda index, carry: (pass_on(index), carry)[1], 0)

    for i in range(PAIRED):
        pltpu.make_async_copy(own.at[2 * mine + i], ownb.at[i, mine], load_sem.at[i]).wait()
    forward_mine(0, 2)

    @pl.when(turn == 0)
    def _():
        hand_over(1)

    forward_mine(2, 3)

    @pl.when(turn == 1)
    def _():
        for i in range(PAIRED):
            hand_over(i)

    forward_other([0, 1], True)
    forward_other([2], False)
    screen(0)
    give_back([0], other)

    @pl.when(turn == 1)
    def _():
        give_back([0], mine)

    forward_mine(3, 4)
    forward_other([3], False)
    screen(1)
    give_back([1], other)

    @pl.when(turn == 1)
    def _():
        give_back([1], mine)

    back_other([0])

    @pl.when(turn == 1)
    def _():
        back_mine(0)

    screen(2)
    screen(3)
    give_back([2, 3], other)

    @pl.when(turn == 0)
    def _():
        give_back([0], mine)
        give_back([1], mine)

    give_back([2], mine)
    give_back([3], mine)
    back_other([1])

    @pl.when(turn == 1)
    def _():
        back_mine(1)

    back_other([2, 3])

    @pl.when(turn == 0)
    def _():
        back_mine(0)
        back_mine(1)

    back_mine(2)
    back_mine(3)

    @pl.when(turn == 1)
    def _():
        settle(VIS - 1, 3)

    def all_of(count, send_sem, recv_sem):
        whole = rows(send, 0, count)
        return remote(whole, whole, send_sem, recv_sem, partner)

    row_share = (ROW - 1) * PAIRED * 2 * VIS * BLOCK
    all_of(row_share, fwd_send, out_recv).wait_send()
    all_of(row_share, bwd_send, out_recv).wait_send()
    visit_share, own_share = VIS * LOCAL * N, PAIRED * LOCAL * N
    for sem in (vis_send, relay_send, part_send):
        all_of(visit_share, sem, out_recv).wait_send()
    all_of(own_share, exch_send, out_recv).wait_send()
    all_of(visit_share, out_send, out_recv).wait()
    all_of(own_share, ret_send, ret_recv).wait()
    for i in range(PAIRED):
        for q in range(4):
            stored(i, q).wait()


def body(own_bands, travel_bands):
    table_list = [jnp.asarray(t) for t in tables()]
    whole = 4 * PAIR_ROWS * PAIRED
    dma = pltpu.SemaphoreType.DMA
    any_space = pl.BlockSpec(memory_space=pl.ANY)
    vmem = pl.BlockSpec(memory_space=pltpu.VMEM)
    return pl.pallas_call(
        kernel,
        out_shape=[
            jax.ShapeDtypeStruct(own_bands.shape, F32),
            jax.ShapeDtypeStruct(travel_bands.shape, F32),
        ],
        in_specs=[any_space, any_space] + [vmem] * 4,
        out_specs=[any_space, any_space],
        scratch_shapes=[
            pltpu.VMEM((PAIRED, 2, LOCAL, N, N), F32),
            pltpu.VMEM((VIS, 2, LOCAL, N, N), F32),
            pltpu.VMEM((whole, N), F32),
            pltpu.VMEM((whole, N), F32),
            pltpu.VMEM((whole, N), F32),
            pltpu.VMEM((PAIRED, 2, LOCAL, N, N), F32),
            pltpu.VMEM((VIS, 2, LOCAL, N, N), F32),
            pltpu.VMEM((VIS, LOCAL, N, N), F32),
            pltpu.VMEM((KYS // 2, N, 2 * N), F32),
            dma((PAIRED,)),
            dma,
            dma((PAIRED, 4)),
            dma,
            dma((VIS, 4)),
            dma,
            dma((VIS, 4)),
            dma,
            dma((VIS, 2)),
            dma,
            dma((VIS, 2, 4)),
            dma,
            dma((VIS, 4)),
            dma,
            dma,
            dma,
            dma,
            dma((PAIRED, 4)),
        ],
        compiler_params=pltpu.CompilerParams(
            collective_id=0, has_side_effects=True, vmem_limit_bytes=46 * 2**20
        ),
        name="exchange_terms",
    )(own_bands, travel_bands, *table_list)


def solution(mesh):
    in_specs = (P("band", "grid", None, None), P("band", "grid", None, None))
    out_specs = (P("band", "grid", None, None), P("band", "grid", None, None))
    return jax.shard_map(body, mesh=mesh, in_specs=in_specs, out_specs=out_specs, check_vma=False)
```

```python
import functools
import math

import jax
import jax.numpy as jnp
import ml_dtypes
import numpy as np
from jax import lax
from jax.experimental import pallas as pl
from jax.experimental.pallas import tpu as pltpu
from jax.sharding import PartitionSpec as P

N = 128
FRACTION = 0.25
ROW = 8
KYS = N // ROW
LOCAL = 8
COLUMN = 8
AHEAD = 1
VIS = 4
PAIRED = 2
BLOCK = LOCAL * KYS
PAIR_ROWS = 2 * ROW * BLOCK
STEPS = ((2, 0), (2, 1), (1, 0), (3, 0), (1, 1), (3, 1), (0, 1))
F32 = jnp.float32
BF16 = jnp.bfloat16
MESH = pl.DeviceIdType.MESH


def real_basis():
    n = np.arange(N)
    rows = []
    for m in range(N):
        if m <= N // 2:
            row = np.cos(2.0 * np.pi * ((m * n) % N) / N)
        else:
            row = np.sin(2.0 * np.pi * (((N - m) * n) % N) / N)
        scale = 1.0 / N if m in (0, N // 2) else 2.0 / N
        rows.append(np.sqrt(scale) * row)
    return np.stack(rows)


def high_low(table):
    high = table.astype(np.float32).astype(ml_dtypes.bfloat16)
    low = (table - high.astype(np.float64)).astype(np.float32).astype(ml_dtypes.bfloat16)
    return high, low


def tables():
    basis = real_basis()
    high, low = high_low(basis)
    high_t, low_t = high.T, low.T
    from_left = np.block([[high, high], [low, low]])
    from_left_inverse = np.block([[high_t, high_t], [low_t, low_t]])
    from_right = np.block([[high_t, low_t], [high_t, low_t]])
    from_right_inverse = np.block([[high, low], [high, low]])
    return [from_left, from_left_inverse, from_right, from_right_inverse]


def halves(value, axis):
    high = value.astype(BF16)
    low = (value - high.astype(F32)).astype(BF16)
    return jnp.concatenate([high, low], axis=axis)


def along_rows(table, value):
    both = jnp.dot(table, halves(value, 0), preferred_element_type=F32)
    return both[:N] + both[N:]


def along_lanes(value, table):
    both = jnp.dot(halves(value, 1), table, preferred_element_type=F32)
    return both[:, :N] + both[:, N:]


def wave_square(position):
    position = lax.rem(position + N // 2, N) - N // 2
    number = 2.0 * math.pi / N * position.astype(F32)
    return number * number


def kernel(
    own, travel, tables_in, own_out, held_out, table,
    ownb, visb, send, recv, back, own_sum, held, held_part, coulomb,
    table_sem, load_sem, exch_send, exch_recv, vis_send, vis_recv, relay_send, relay_recv,
    fwd_send, fwd_recv, bwd_send, bwd_recv,
    part_send, part_recv, out_send, out_recv, ret_send, ret_recv, store_sem,
):
    band = lax.axis_index("band")
    groups = lax.axis_size("band")
    grid = lax.axis_index("grid")
    mine = grid // ROW
    other = 1 - mine
    place = grid % ROW
    x, core = place // 2, place % 2
    partner = {"grid": other * ROW + place}
    ahead_band = (band + 1) % groups
    turn = (COLUMN - band % COLUMN) // COLUMN
    ahead_turn = (COLUMN - ahead_band % COLUMN) // COLUMN
    direct = (mine + turn) % 2
    passed = 1 - direct
    ahead = {"band": ahead_band, "grid": (mine + ahead_turn) % 2 * ROW + place}
    behind = {"band": (band + groups - 1) % groups, "grid": direct * ROW + place}
    places = [((x + dx) % 4) * 2 + (core + dc) % 2 for dx, dc in STEPS]
    peers = [{"grid": mine * ROW + p} for p in places]

    def remote(src, dst, send_sem, recv_sem, device):
        return pltpu.make_async_remote_copy(
            src_ref=src, dst_ref=dst, send_sem=send_sem, recv_sem=recv_sem,
            device_id=device, device_id_type=MESH,
        )

    lt_ref, lti_ref, wx_ref, wxi_ref = (table.at[n] for n in range(4))
    pltpu.make_async_copy(tables_in, table, table_sem).start()
    for i in range(PAIRED):
        pltpu.make_async_copy(own.at[2 * mine + i], ownb.at[i, mine], load_sem.at[i]).start()

    barrier = pltpu.get_barrier_semaphore()
    for device in [ahead, behind, partner] + peers:
        pl.semaphore_signal(barrier, inc=1, device_id=device, device_id_type=MESH)
    pl.semaphore_wait(barrier, 3 + len(peers))

    def visitor(j, q):
        return remote(
            travel.at[j, pl.ds(2 * q, 2)], visb.at[j, mine, pl.ds(2 * q, 2)],
            vis_send, vis_recv.at[j, q], ahead,
        )

    def relay(j, q, half):
        return remote(
            visb.at[j, half, pl.ds(2 * q, 2)], visb.at[j, half, pl.ds(2 * q, 2)],
            relay_send, relay_recv.at[j, q], partner,
        )

    def exchange(i, q, half, index):
        return remote(
            own.at[index, pl.ds(2 * q, 2)], ownb.at[i, half, pl.ds(2 * q, 2)],
            exch_send, exch_recv.at[i, q], partner,
        )

    def hand_over(i):
        for q in range(4):
            exchange(i, q, mine, 2 * other + i).start()

    for j in range(VIS):
        for q in range(4):
            visitor(j, q).start()

    @pl.when(turn == 0)
    def _():
        hand_over(0)

    kz = lax.broadcasted_iota(jnp.int32, (N, 2 * N), 0)
    lane = lax.broadcasted_iota(jnp.int32, (N, 2 * N), 1)
    kx_square = wave_square(lax.rem(lane, N))
    kz_square = wave_square(kz)

    def fill(kp, carry):
        ky = place * KYS + 2 * kp + lane // N
        squared = kz_square + wave_square(ky) + kx_square
        safe = jnp.where(squared > 0.0, squared, 1.0)
        value = jnp.where(squared > 0.0, 4.0 * math.pi / safe, 0.0)
        coulomb[kp] = -FRACTION * value
        return carry

    lax.fori_loop(0, KYS // 2, fill, 0)

    def base(j, i, half, p):
        return ((j * PAIRED + i) * 2 + half) * ROW * BLOCK + p * BLOCK

    def rows(ref, start, count):
        return ref.at[pl.ds(pl.multiple_of(start, KYS), count)]

    def pass_on(index):
        j, q = index // 4, index % 4
        visitor(j, q).wait_recv()
        relay(j, q, direct).start()

    def transform(j, i, half, q):
        planes = pl.ds(2 * q, 2)
        density = (ownb[i, half, planes] * visb[j, half, planes]).reshape(2 * N, N)
        wave = along_lanes(density, wx_ref[...])
        wave = jnp.concatenate([wave[:N], wave[N:]], axis=1)
        wave = along_rows(lt_ref[...], wave)
        for p in range(ROW):
            for z in range(2):
                start = base(j, i, half, p) + (2 * q + z) * KYS
                send[pl.ds(pl.multiple_of(start, KYS), KYS), :] = wave[
                    p * KYS : (p + 1) * KYS, z * N : (z + 1) * N
                ]
        start = pl.multiple_of(base(j, i, half, place) + 2 * q * KYS, KYS)
        recv[pl.ds(start, 2 * KYS), :] = send[pl.ds(start, 2 * KYS), :]
        for p, peer in zip(places, peers):
            remote(
                rows(send, base(j, i, half, p) + 2 * q * KYS, 2 * KYS),
                rows(recv, base(j, i, half, place) + 2 * q * KYS, 2 * KYS),
                fwd_send, fwd_recv.at[j, half], peer,
            ).start()

    def forward_mine(first, last):
        def piece(step, carry):
            j, q = step // 4, step % 4
            index = step + AHEAD * turn

            @pl.when(index < 4 * VIS)
            def _():
                pass_on(index)

            @pl.when(turn == 1)
            def _():
                relay(j, q, passed).wait_recv()

            for i in range(PAIRED):
                transform(j, i, mine, q)
            return carry

        lax.fori_loop(4 * first, 4 * last, piece, 0)

    def forward_other(visitors, fresh):
        def piece(step, carry):
            i, q = step // 4, step % 4
            if fresh:
                exchange(i, q, other, 2 * mine + i).wait_recv()

            @pl.when((turn == 0) & (i == 0))
            def _():
                for j in visitors:
                    relay(j, q, passed).wait_recv()

            for j in visitors:
                transform(j, i, other, q)
            return carry

        lax.fori_loop(0, 4 * PAIRED, piece, 0)

    def screen(j):
        for half in (mine, other):
            whole = rows(recv, 0, (ROW - 1) * PAIRED * BLOCK)
            remote(whole, whole, fwd_send, fwd_recv.at[j, half], partner).wait_recv()

        def columns(step, carry):
            i, kp = step // (KYS // 2), step % (KYS // 2)
            start = (j * PAIRED + i) * PAIR_ROWS + 2 * kp
            first = pl.ds(start, N, stride=KYS)
            second = pl.ds(start + 1, N, stride=KYS)
            wave = jnp.concatenate([recv[first, :], recv[second, :]], axis=1)
            wave = along_rows(lt_ref[...], wave) * coulomb[kp]
            wave = along_rows(lti_ref[...], wave)
            recv[first, :] = wave[:, :N]
            recv[second, :] = wave[:, N:]
            return carry

        lax.fori_loop(0, PAIRED * KYS // 2, columns, 0)
        for i in range(PAIRED):
            for half in range(2):
                start = pl.multiple_of(base(j, i, half, place), KYS)
                back[pl.ds(start, BLOCK), :] = recv[pl.ds(start, BLOCK), :]

    def give_back(visitors, half):
        def piece(q, carry):
            for j in visitors:
                for i in range(PAIRED):
                    for p, peer in zip(places, peers):
                        remote(
                            rows(recv, base(j, i, half, p) + 2 * q * KYS, 2 * KYS),
                            rows(back, base(j, i, half, place) + 2 * q * KYS, 2 * KYS),
                            bwd_send, bwd_recv.at[j, half, q], peer,
                        ).start()
            return carry

        lax.fori_loop(0, 4, piece, 0)

    def inverse(j, half, q):
        whole = rows(back, 0, (ROW - 1) * PAIRED * 2 * KYS)
        remote(whole, whole, bwd_send, bwd_recv.at[j, half, q], partner).wait_recv()
        planes = pl.ds(2 * q, 2)
        held_term = None
        for i in range(PAIRED):
            sides = []
            for k in range(2):
                parts = []
                for p in range(ROW):
                    start = base(j, i, half, p) + (2 * q + k) * KYS
                    parts.append(back[pl.ds(pl.multiple_of(start, KYS), KYS), :])
                sides.append(jnp.concatenate(parts, axis=0))
            wave = along_rows(lti_ref[...], jnp.concatenate(sides, axis=1))
            wave = jnp.concatenate([wave[:, :N], wave[:, N:]], axis=0)
            potential = along_lanes(wave, wxi_ref[...]).reshape(2, N, N)
            own_part = potential * visb[j, half, planes]
            if j > 0:
                own_part = own_part + own_sum[i, half, planes]
            own_sum[i, half, planes] = own_part
            term = potential * ownb[i, half, planes]
            held_term = term if held_term is None else held_term + term
        held[j, half, planes] = held_term

    def partial(j, q):
        planes = pl.ds(2 * q, 2)
        return remote(
            held.at[j, passed, planes], held_part.at[j, planes],
            part_send, part_recv.at[j, q], partner,
        )

    def outgoing(j, q):
        planes = pl.ds(2 * q, 2)
        return remote(
            held.at[j, direct, planes], held_out.at[j, planes],
            out_send, out_recv, behind,
        )

    def returned(i, q):
        planes = pl.ds(2 * q, 2)
        return remote(
            own_sum.at[i, other, planes], own_out.at[2 * mine + i, planes],
            ret_send, ret_recv, partner,
        )

    def stored(i, q):
        planes = pl.ds(2 * q, 2)
        return pltpu.make_async_copy(
            own_sum.at[i, mine, planes], own_out.at[2 * mine + i, planes], store_sem.at[i, q]
        )

    def settle(j, q):
        partial(j, q).wait_recv()
        planes = pl.ds(2 * q, 2)
        held[j, direct, planes] = held[j, direct, planes] + held_part[j, planes]
        outgoing(j, q).start()

    def back_other(visitors):
        def piece(q, carry):
            for j in visitors:
                inverse(j, other, q)

                @pl.when(turn == 0)
                def _():
                    partial(j, q).start()

            if VIS - 1 in visitors:
                for i in range(PAIRED):
                    returned(i, q).start()
            return carry

        lax.fori_loop(0, 4, piece, 0)

    def back_mine(j):
        def piece(q, carry):
            inverse(j, mine, q)
            if j == VIS - 1:
                for i in range(PAIRED):
                    stored(i, q).start()

            @pl.when(turn == 1)
            def _():
                partial(j, q).start()

            index = 4 * j + q - turn

            @pl.when(index >= 0)
            def _():
                settle(index // 4, index % 4)

            return carry

        lax.fori_loop(0, 4, piece, 0)

    @pl.when(turn == 1)
    def _():
        lax.fori_loop(0, AHEAD, lambda index, carry: (pass_on(index), carry)[1], 0)

    pltpu.make_async_copy(tables_in, table, table_sem).wait()
    for i in range(PAIRED):
        pltpu.make_async_copy(own.at[2 * mine + i], ownb.at[i, mine], load_sem.at[i]).wait()
    forward_mine(0, 2)

    @pl.when(turn == 0)
    def _():
        hand_over(1)

    forward_mine(2, 3)

    @pl.when(turn == 1)
    def _():
        for i in range(PAIRED):
            hand_over(i)

    forward_other([0, 1], True)
    forward_other([2], False)
    screen(0)
    give_back([0], other)

    @pl.when(turn == 1)
    def _():
        give_back([0], mine)

    forward_mine(3, 4)
    forward_other([3], False)
    screen(1)
    give_back([1], other)

    @pl.when(turn == 1)
    def _():
        give_back([1], mine)

    back_other([0])

    @pl.when(turn == 1)
    def _():
        back_mine(0)

    screen(2)
    screen(3)
    give_back([2, 3], other)

    @pl.when(turn == 0)
    def _():
        give_back([0], mine)
        give_back([1], mine)

    give_back([2], mine)
    give_back([3], mine)
    back_other([1])

    @pl.when(turn == 1)
    def _():
        back_mine(1)

    back_other([2, 3])

    @pl.when(turn == 0)
    def _():
        back_mine(0)
        back_mine(1)

    back_mine(2)
    back_mine(3)

    @pl.when(turn == 1)
    def _():
        settle(VIS - 1, 3)

    def all_of(count, send_sem, recv_sem):
        whole = rows(send, 0, count)
        return remote(whole, whole, send_sem, recv_sem, partner)

    row_share = (ROW - 1) * PAIRED * 2 * VIS * BLOCK
    all_of(row_share, fwd_send, out_recv).wait_send()
    all_of(row_share, bwd_send, out_recv).wait_send()
    visit_share, own_share = VIS * LOCAL * N, PAIRED * LOCAL * N
    for sem in (vis_send, relay_send, part_send):
        all_of(visit_share, sem, out_recv).wait_send()
    all_of(own_share, exch_send, out_recv).wait_send()
    all_of(visit_share, out_send, out_recv).wait()
    all_of(own_share, ret_send, ret_recv).wait()
    for i in range(PAIRED):
        for q in range(4):
            stored(i, q).wait()


def body(own_bands, travel_bands):
    table_stack = jnp.asarray(np.stack(tables()))
    whole = 4 * PAIR_ROWS * PAIRED
    dma = pltpu.SemaphoreType.DMA
    any_space = pl.BlockSpec(memory_space=pl.ANY)
    return pl.pallas_call(
        kernel,
        out_shape=[
            jax.ShapeDtypeStruct(own_bands.shape, F32),
            jax.ShapeDtypeStruct(travel_bands.shape, F32),
        ],
        in_specs=[any_space] * 3,
        out_specs=[any_space, any_space],
        scratch_shapes=[
            pltpu.VMEM((4, 2 * N, 2 * N), BF16),
            pltpu.VMEM((PAIRED, 2, LOCAL, N, N), F32),
            pltpu.VMEM((VIS, 2, LOCAL, N, N), F32),
            pltpu.VMEM((whole, N), F32),
            pltpu.VMEM((whole, N), F32),
            pltpu.VMEM((whole, N), F32),
            pltpu.VMEM((PAIRED, 2, LOCAL, N, N), F32),
            pltpu.VMEM((VIS, 2, LOCAL, N, N), F32),
            pltpu.VMEM((VIS, LOCAL, N, N), F32),
            pltpu.VMEM((KYS // 2, N, 2 * N), F32),
            dma,
            dma((PAIRED,)),
            dma,
            dma((PAIRED, 4)),
            dma,
            dma((VIS, 4)),
            dma,
            dma((VIS, 4)),
            dma,
            dma((VIS, 2)),
            dma,
            dma((VIS, 2, 4)),
            dma,
            dma((VIS, 4)),
            dma,
            dma,
            dma,
            dma,
            dma((PAIRED, 4)),
        ],
        compiler_params=pltpu.CompilerParams(
            collective_id=0, has_side_effects=True, vmem_limit_bytes=49 * 2**20
        ),
        name="exchange_terms",
    )(own_bands, travel_bands, table_stack)


def solution(mesh):
    in_specs = (P("band", "grid", None, None), P("band", "grid", None, None))
    out_specs = (P("band", "grid", None, None), P("band", "grid", None, None))
    return jax.shard_map(body, mesh=mesh, in_specs=in_specs, out_specs=out_specs, check_vma=False)
```

```python
import functools
import math

import jax
import jax.numpy as jnp
import ml_dtypes
import numpy as np
from jax import lax
from jax.experimental import pallas as pl
from jax.experimental.pallas import tpu as pltpu
from jax.sharding import PartitionSpec as P

N = 128
FRACTION = 0.25
ROW = 8
KYS = N // ROW
LOCAL = 8
COLUMN = 8
VIS = 4
PAIRED = 2
BLOCK = LOCAL * KYS
PAIR_ROWS = 2 * ROW * BLOCK
STEPS = ((2, 0), (2, 1), (1, 0), (3, 0), (1, 1), (3, 1), (0, 1))
F32 = jnp.float32
BF16 = jnp.bfloat16
MESH = pl.DeviceIdType.MESH


def real_basis():
    n = np.arange(N)
    rows = []
    for m in range(N):
        if m <= N // 2:
            row = np.cos(2.0 * np.pi * ((m * n) % N) / N)
        else:
            row = np.sin(2.0 * np.pi * (((N - m) * n) % N) / N)
        scale = 1.0 / N if m in (0, N // 2) else 2.0 / N
        rows.append(np.sqrt(scale) * row)
    return np.stack(rows)


def high_low(table):
    high = table.astype(np.float32).astype(ml_dtypes.bfloat16)
    low = (table - high.astype(np.float64)).astype(np.float32).astype(ml_dtypes.bfloat16)
    return high, low


def tables():
    basis = real_basis()
    high, low = high_low(basis)
    high_t, low_t = high.T, low.T
    from_left = np.block([[high, high], [low, low]])
    from_left_inverse = np.block([[high_t, high_t], [low_t, low_t]])
    from_right = np.block([[high_t, low_t], [high_t, low_t]])
    from_right_inverse = np.block([[high, low], [high, low]])
    return [from_left, from_left_inverse, from_right, from_right_inverse]


def halves(value, axis):
    high = value.astype(BF16)
    low = (value - high.astype(F32)).astype(BF16)
    return jnp.concatenate([high, low], axis=axis)


def along_rows(table, value):
    both = jnp.dot(table, halves(value, 0), preferred_element_type=F32)
    return both[:N] + both[N:]


def along_lanes(value, table):
    both = jnp.dot(halves(value, 1), table, preferred_element_type=F32)
    return both[:, :N] + both[:, N:]


def wave_square(position):
    position = lax.rem(position + N // 2, N) - N // 2
    number = 2.0 * math.pi / N * position.astype(F32)
    return number * number


def kernel(
    own, travel, tables_in, own_out, held_out, table,
    ownb, visb, send, recv, back, own_sum, held, held_part, coulomb,
    table_sem, load_sem, exch_send, exch_recv, vis_send, vis_recv, relay_send, relay_recv,
    fwd_send, fwd_recv, bwd_send, bwd_recv,
    part_send, part_recv, out_send, out_recv, ret_send, ret_recv, store_sem,
):
    band = lax.axis_index("band")
    groups = lax.axis_size("band")
    grid = lax.axis_index("grid")
    mine = grid // ROW
    other = 1 - mine
    place = grid % ROW
    x, core = place // 2, place % 2
    partner = {"grid": other * ROW + place}
    ahead_band = (band + 1) % groups
    turn = (COLUMN - band % COLUMN) // COLUMN
    ahead_turn = (COLUMN - ahead_band % COLUMN) // COLUMN
    direct = (mine + turn) % 2
    passed = 1 - direct
    ahead = {"band": ahead_band, "grid": (mine + ahead_turn) % 2 * ROW + place}
    behind = {"band": (band + groups - 1) % groups, "grid": direct * ROW + place}
    places = [((x + dx) % 4) * 2 + (core + dc) % 2 for dx, dc in STEPS]
    peers = [{"grid": mine * ROW + p} for p in places]

    def remote(src, dst, send_sem, recv_sem, device):
        return pltpu.make_async_remote_copy(
            src_ref=src, dst_ref=dst, send_sem=send_sem, recv_sem=recv_sem,
            device_id=device, device_id_type=MESH,
        )

    lt_ref, lti_ref, wx_ref, wxi_ref = (table.at[n] for n in range(4))
    pltpu.make_async_copy(tables_in, table, table_sem).start()
    for i in range(PAIRED):
        pltpu.make_async_copy(own.at[2 * mine + i], ownb.at[i, mine], load_sem.at[i]).start()

    barrier = pltpu.get_barrier_semaphore()
    for device in [ahead, behind, partner] + peers:
        pl.semaphore_signal(barrier, inc=1, device_id=device, device_id_type=MESH)
    pl.semaphore_wait(barrier, 3 + len(peers))

    def visitor(j, q):
        return remote(
            travel.at[j, pl.ds(2 * q, 2)], visb.at[j, mine, pl.ds(2 * q, 2)],
            vis_send, vis_recv.at[j, q], ahead,
        )

    def relay(j, q, half):
        return remote(
            visb.at[j, half, pl.ds(2 * q, 2)], visb.at[j, half, pl.ds(2 * q, 2)],
            relay_send, relay_recv.at[j, q], partner,
        )

    def exchange(i, q, half, index):
        return remote(
            own.at[index, pl.ds(2 * q, 2)], ownb.at[i, half, pl.ds(2 * q, 2)],
            exch_send, exch_recv.at[i, q], partner,
        )

    def hand_over(i):
        for q in range(4):
            exchange(i, q, mine, 2 * other + i).start()

    for j in range(VIS):
        for q in range(4):
            visitor(j, q).start()

    @pl.when(turn == 0)
    def _():
        hand_over(0)

    @pl.when(turn == 1)
    def _():
        for q in range(4):
            for i in range(PAIRED):
                exchange(i, q, mine, 2 * other + i).start()

    kz = lax.broadcasted_iota(jnp.int32, (N, 2 * N), 0)
    lane = lax.broadcasted_iota(jnp.int32, (N, 2 * N), 1)
    kx_square = wave_square(lax.rem(lane, N))
    kz_square = wave_square(kz)

    def fill(kp, carry):
        ky = place * KYS + 2 * kp + lane // N
        squared = kz_square + wave_square(ky) + kx_square
        safe = jnp.where(squared > 0.0, squared, 1.0)
        value = jnp.where(squared > 0.0, 4.0 * math.pi / safe, 0.0)
        coulomb[kp] = -FRACTION * value
        return carry

    lax.fori_loop(0, KYS // 2, fill, 0)

    def base(j, i, half, p):
        return ((j * PAIRED + i) * 2 + half) * ROW * BLOCK + p * BLOCK

    def rows(ref, start, count):
        return ref.at[pl.ds(pl.multiple_of(start, KYS), count)]

    def pass_on(index):
        j, q = index // 4, index % 4
        visitor(j, q).wait_recv()
        relay(j, q, direct).start()

    def transform(j, i, half, q):
        planes = pl.ds(2 * q, 2)
        density = (ownb[i, half, planes] * visb[j, half, planes]).reshape(2 * N, N)
        wave = along_lanes(density, wx_ref[...])
        wave = jnp.concatenate([wave[:N], wave[N:]], axis=1)
        wave = along_rows(lt_ref[...], wave)
        for p in range(ROW):
            for z in range(2):
                start = base(j, i, half, p) + (2 * q + z) * KYS
                send[pl.ds(pl.multiple_of(start, KYS), KYS), :] = wave[
                    p * KYS : (p + 1) * KYS, z * N : (z + 1) * N
                ]
        start = pl.multiple_of(base(j, i, half, place) + 2 * q * KYS, KYS)
        recv[pl.ds(start, 2 * KYS), :] = send[pl.ds(start, 2 * KYS), :]
        for p, peer in zip(places, peers):
            remote(
                rows(send, base(j, i, half, p) + 2 * q * KYS, 2 * KYS),
                rows(recv, base(j, i, half, place) + 2 * q * KYS, 2 * KYS),
                fwd_send, fwd_recv.at[j, half], peer,
            ).start()

    def forward_mine(first, last):
        def piece(step, carry):
            j, q = step // 4, step % 4
            pass_on(step)
            for i in range(PAIRED):
                transform(j, i, mine, q)
            return carry

        lax.fori_loop(4 * first, 4 * last, piece, 0)

    def turned_start():
        def piece(q, carry):
            pass_on(q)
            for i in range(PAIRED):
                exchange(i, q, other, 2 * mine + i).wait_recv()
                transform(0, i, other, q)

            @pl.when(q > 0)
            def _():
                straight(q + 3, 0)

            return carry

        def straight(step, carry):
            pass_on(step)
            for i in range(PAIRED):
                transform(step // 4, i, other, step % 4)
            return carry

        def own_planes(step, carry):
            relay(step // 4, step % 4, passed).wait_recv()
            for i in range(PAIRED):
                transform(step // 4, i, mine, step % 4)
            return carry

        lax.fori_loop(0, 4, piece, 0)
        lax.fori_loop(7, 12, straight, 0)
        lax.fori_loop(0, 12, own_planes, 0)

    def turned(first, last):
        def own_planes(step):
            relay(step // 4, step % 4, passed).wait_recv()
            for i in range(PAIRED):
                transform(step // 4, i, mine, step % 4)

        def piece(step, carry):
            pass_on(step)
            for i in range(PAIRED):
                transform(step // 4, i, other, step % 4)

            @pl.when(step > 4 * first)
            def _():
                own_planes(step - 1)

            return carry

        lax.fori_loop(4 * first, 4 * last, piece, 0)
        own_planes(4 * last - 1)

    def forward_other(visitors, fresh):
        def piece(step, carry):
            i, q = step // 4, step % 4
            if fresh:
                exchange(i, q, other, 2 * mine + i).wait_recv()

            @pl.when(i == 0)
            def _():
                for j in visitors:
                    relay(j, q, passed).wait_recv()

            for j in visitors:
                transform(j, i, other, q)
            return carry

        lax.fori_loop(0, 4 * PAIRED, piece, 0)

    def screen(j):
        for half in (mine, other):
            whole = rows(recv, 0, (ROW - 1) * PAIRED * BLOCK)
            remote(whole, whole, fwd_send, fwd_recv.at[j, half], partner).wait_recv()

        def columns(step, carry):
            i, kp = step // (KYS // 2), step % (KYS // 2)
            start = (j * PAIRED + i) * PAIR_ROWS + 2 * kp
            first = pl.ds(start, N, stride=KYS)
            second = pl.ds(start + 1, N, stride=KYS)
            wave = jnp.concatenate([recv[first, :], recv[second, :]], axis=1)
            wave = along_rows(lt_ref[...], wave) * coulomb[kp]
            wave = along_rows(lti_ref[...], wave)
            recv[first, :] = wave[:, :N]
            recv[second, :] = wave[:, N:]
            return carry

        lax.fori_loop(0, PAIRED * KYS // 2, columns, 0)
        for i in range(PAIRED):
            for half in range(2):
                start = pl.multiple_of(base(j, i, half, place), KYS)
                back[pl.ds(start, BLOCK), :] = recv[pl.ds(start, BLOCK), :]

    def give_back(visitors, half):
        def piece(q, carry):
            for j in visitors:
                for i in range(PAIRED):
                    for p, peer in zip(places, peers):
                        remote(
                            rows(recv, base(j, i, half, p) + 2 * q * KYS, 2 * KYS),
                            rows(back, base(j, i, half, place) + 2 * q * KYS, 2 * KYS),
                            bwd_send, bwd_recv.at[j, half, q], peer,
                        ).start()
            return carry

        lax.fori_loop(0, 4, piece, 0)

    def inverse(j, half, q):
        whole = rows(back, 0, (ROW - 1) * PAIRED * 2 * KYS)
        remote(whole, whole, bwd_send, bwd_recv.at[j, half, q], partner).wait_recv()
        planes = pl.ds(2 * q, 2)
        held_term = None
        for i in range(PAIRED):
            sides = []
            for k in range(2):
                parts = []
                for p in range(ROW):
                    start = base(j, i, half, p) + (2 * q + k) * KYS
                    parts.append(back[pl.ds(pl.multiple_of(start, KYS), KYS), :])
                sides.append(jnp.concatenate(parts, axis=0))
            wave = along_rows(lti_ref[...], jnp.concatenate(sides, axis=1))
            wave = jnp.concatenate([wave[:, :N], wave[:, N:]], axis=0)
            potential = along_lanes(wave, wxi_ref[...]).reshape(2, N, N)
            own_part = potential * visb[j, half, planes]
            if j > 0:
                own_part = own_part + own_sum[i, half, planes]
            own_sum[i, half, planes] = own_part
            term = potential * ownb[i, half, planes]
            held_term = term if held_term is None else held_term + term
        held[j, half, planes] = held_term

    def partial(j, q):
        planes = pl.ds(2 * q, 2)
        return remote(
            held.at[j, passed, planes], held_part.at[j, planes],
            part_send, part_recv.at[j, q], partner,
        )

    def outgoing(j, q):
        planes = pl.ds(2 * q, 2)
        return remote(
            held.at[j, direct, planes], held_out.at[j, planes],
            out_send, out_recv, behind,
        )

    def returned(i, q):
        planes = pl.ds(2 * q, 2)
        return remote(
            own_sum.at[i, other, planes], own_out.at[2 * mine + i, planes],
            ret_send, ret_recv, partner,
        )

    def stored(i, q):
        planes = pl.ds(2 * q, 2)
        return pltpu.make_async_copy(
            own_sum.at[i, mine, planes], own_out.at[2 * mine + i, planes], store_sem.at[i, q]
        )

    def settle(j, q):
        partial(j, q).wait_recv()
        planes = pl.ds(2 * q, 2)
        held[j, direct, planes] = held[j, direct, planes] + held_part[j, planes]
        outgoing(j, q).start()

    def back_other(visitors, turned_here):
        def piece(q, carry):
            for j in visitors:
                inverse(j, other, q)
                if not turned_here:
                    partial(j, q).start()
            if VIS - 1 in visitors:
                for i in range(PAIRED):
                    returned(i, q).start()
            if turned_here:
                for j in visitors:
                    settle(j, q)
            return carry

        lax.fori_loop(0, 4, piece, 0)

    def back_mine(j, turned_here):
        def piece(q, carry):
            inverse(j, mine, q)
            if turned_here:
                partial(j, q).start()
            else:
                settle(j, q)
            if j == VIS - 1:
                for i in range(PAIRED):
                    stored(i, q).start()
            return carry

        lax.fori_loop(0, 4, piece, 0)

    pltpu.make_async_copy(tables_in, table, table_sem).wait()
    for i in range(PAIRED):
        pltpu.make_async_copy(own.at[2 * mine + i], ownb.at[i, mine], load_sem.at[i]).wait()
    @pl.when(turn == 0)
    def _():
        forward_mine(0, 2)
        hand_over(1)
        forward_mine(2, 3)
        forward_other([0, 1], True)
        forward_other([2], False)
        screen(0)
        give_back([0], other)
        forward_mine(3, 4)
        forward_other([3], False)
        screen(1)
        give_back([1], other)
        back_other([0], False)
        screen(2)
        screen(3)
        give_back([2, 3], other)
        for j in range(VIS):
            give_back([j], mine)
        back_other([1], False)
        back_other([2, 3], False)
        for j in range(VIS):
            back_mine(j, False)

    @pl.when(turn == 1)
    def _():
        turned_start()
        screen(0)
        give_back([0], mine)
        give_back([0], other)
        turned(3, 4)
        screen(1)
        give_back([1], mine)
        back_mine(0, True)
        screen(2)
        give_back([2], mine)
        back_other([0], True)
        screen(3)
        give_back([3], mine)
        give_back([1, 2, 3], other)
        for j in range(1, VIS):
            back_mine(j, True)
        back_other([1, 2, 3], True)

    def all_of(count, send_sem, recv_sem):
        whole = rows(send, 0, count)
        return remote(whole, whole, send_sem, recv_sem, partner)

    row_share = (ROW - 1) * PAIRED * 2 * VIS * BLOCK
    all_of(row_share, fwd_send, out_recv).wait_send()
    all_of(row_share, bwd_send, out_recv).wait_send()
    visit_share, own_share = VIS * LOCAL * N, PAIRED * LOCAL * N
    for sem in (vis_send, relay_send, part_send):
        all_of(visit_share, sem, out_recv).wait_send()
    all_of(own_share, exch_send, out_recv).wait_send()
    all_of(visit_share, out_send, out_recv).wait()
    all_of(own_share, ret_send, ret_recv).wait()
    for i in range(PAIRED):
        for q in range(4):
            stored(i, q).wait()


def body(own_bands, travel_bands):
    table_stack = jnp.asarray(np.stack(tables()))
    whole = 4 * PAIR_ROWS * PAIRED
    dma = pltpu.SemaphoreType.DMA
    any_space = pl.BlockSpec(memory_space=pl.ANY)
    return pl.pallas_call(
        kernel,
        out_shape=[
            jax.ShapeDtypeStruct(own_bands.shape, F32),
            jax.ShapeDtypeStruct(travel_bands.shape, F32),
        ],
        in_specs=[any_space] * 3,
        out_specs=[any_space, any_space],
        scratch_shapes=[
            pltpu.VMEM((4, 2 * N, 2 * N), BF16),
            pltpu.VMEM((PAIRED, 2, LOCAL, N, N), F32),
            pltpu.VMEM((VIS, 2, LOCAL, N, N), F32),
            pltpu.VMEM((whole, N), F32),
            pltpu.VMEM((whole, N), F32),
            pltpu.VMEM((whole, N), F32),
            pltpu.VMEM((PAIRED, 2, LOCAL, N, N), F32),
            pltpu.VMEM((VIS, 2, LOCAL, N, N), F32),
            pltpu.VMEM((VIS, LOCAL, N, N), F32),
            pltpu.VMEM((KYS // 2, N, 2 * N), F32),
            dma,
            dma((PAIRED,)),
            dma,
            dma((PAIRED, 4)),
            dma,
            dma((VIS, 4)),
            dma,
            dma((VIS, 4)),
            dma,
            dma((VIS, 2)),
            dma,
            dma((VIS, 2, 4)),
            dma,
            dma((VIS, 4)),
            dma,
            dma,
            dma,
            dma,
            dma((PAIRED, 4)),
        ],
        compiler_params=pltpu.CompilerParams(
            collective_id=0, has_side_effects=True, vmem_limit_bytes=49 * 2**20
        ),
        name="exchange_terms",
    )(own_bands, travel_bands, table_stack)


def solution(mesh):
    in_specs = (P("band", "grid", None, None), P("band", "grid", None, None))
    out_specs = (P("band", "grid", None, None), P("band", "grid", None, None))
    return jax.shard_map(body, mesh=mesh, in_specs=in_specs, out_specs=out_specs, check_vma=False)
```
